32 devices in a mesh: dp: 2 (over z, core), tp: 16 (over x, y).
Axes of the slice: x: 4, y: 4, z: 1, core: 2. Of those that a mesh axis runs over, the one named last changes fastest.
The devices are a block of a 4x4x8 slice.
Arguments:
- x: bfloat16 [7168, 5120], P(('dp', 'tp')), parts along dimension 0
- dy: bfloat16 [7168, 5120], P(('dp', 'tp')), parts along dimension 0
- pre: bfloat16 [7168, 20480], P('dp', 'tp'), parts along dimension 0
- w_in: bfloat16 [5120, 20480], P(None, 'tp')
- w_down: bfloat16 [20480, 5120], P('tp')
Outputs:
- output 1: bfloat16 [7168, 5120], P(('dp', 'tp')), parts along dimension 0
- output 2: bfloat16 [10240, 20480], P('dp', 'tp'), parts along dimension 0
- output 3: bfloat16 [40960, 5120], P(('dp', 'tp')), parts along dimension 0
There are 2 independent parts. The reference program is written for one: setup_inputs(seed, part) draws one part's arguments, and reference() takes and returns one part's arrays. A program takes and returns all parts, laid end to end along the dimension named above; an argument that names none is the same for every part.
All inputs are finite; a program needn't handle non-finite values.
Results may differ from the reference program's by a relative error of at most 0.012.
Values are sent between devices in bfloat16 or wider.
A program may use at most 768 MiB of HBM per device.

```python
import jax
import jax.numpy as jnp

ROWS = 3584
D = 5120
FF = 20480


def act(pre):
    return jax.nn.gelu(pre)


def setup_inputs(seed: int = 0, part: int = 0) -> dict:
    kx, ky, ka, ki, kd = jax.random.split(jax.random.key(seed), 5)
    kx, ky, ka = (jax.random.fold_in(k, part) for k in (kx, ky, ka))
    drawn = {
        "x": jax.random.normal(kx, (ROWS, D), jnp.float32),
        "dy": jax.random.normal(ky, (ROWS, D), jnp.float32),
        "pre": jax.random.normal(ka, (ROWS, FF), jnp.float32),
        "w_in": jax.random.normal(ki, (D, FF), jnp.float32) * D**-0.5,
        "w_down": jax.random.normal(kd, (FF, D), jnp.float32) * FF**-0.5,
    }
    return {k: v.astype(jnp.bfloat16) for k, v in drawn.items()}


def reference(x, dy, pre, w_in, w_down):
    hidden, back = jax.vjp(act, pre.astype(jnp.float32))
    d_hidden = jnp.dot(dy, w_down.T, preferred_element_type=jnp.float32)
    d_pre = back(d_hidden)[0].astype(jnp.bfloat16)
    dx = jnp.dot(d_pre, w_in.T, preferred_element_type=jnp.float32)
    dw_in = jnp.dot(x.T, d_pre, preferred_element_type=jnp.float32)
    dw_down = jnp.dot(hidden.astype(jnp.bfloat16).T, dy, preferred_element_type=jnp.float32)
    return tuple(g.astype(jnp.bfloat16) for g in (dx, dw_in, dw_down))
```

```python
import functools
import math

import jax
import jax.numpy as jnp
from jax import lax
from jax.experimental import pallas as pl
from jax.experimental.pallas import tpu as pltpu

P = jax.sharding.PartitionSpec
MESH = pl.DeviceIdType.MESH
F32, BF16 = jnp.float32, jnp.bfloat16
RINGS = ((0, 1), (0, -1), (1, 1), (1, -1))
PIECES = 2
CHUNK = 512
SUB = 256


def act(pre):
    return jax.nn.gelu(pre)


def position(cycle, me, k):
    x, y = me // k, lax.rem(me, k)
    return (x if cycle == 0 else y) * k + lax.rem(x + y, k)


def device(cycle, pos, k):
    n = k * k
    pos = lax.rem(pos + 4 * n, n)
    a, b = pos // k, lax.rem(pos, k)
    m = lax.rem(b - a + k, k)
    return a * k + m if cycle == 0 else m * k + a


def at(i, size):
    return pl.ds(pl.multiple_of(i * size, size), size)


NT = (((1,), (1,)), ((), ()))
NN = (((1,), (0,)), ((), ()))


def kernel(
    n, x, dy, pre, w_in, w_down, dx, dw_in, dw_down, gx, gy, land,
    w, d_pre, turned, wide, pre_in, tall, out_a, out_b, term,
    send, recv, rs_send, rs_recv, w_sem, wide_sem, tall_sem, out_sem, fetch_sem,
):
    k = math.isqrt(n)
    rows, d = x.shape
    tokens, ff = d_pre.shape
    quarter = d // len(RINGS)
    piece = quarter // PIECES
    half = rows // PIECES
    rings = range(len(RINGS))
    me = lax.axis_index("tp")
    pos = [position(cycle, me, k) for cycle, _ in RINGS]
    ahead = [device(c, pos[r] + way, k) for r, (c, way) in enumerate(RINGS)]

    barrier = pltpu.get_barrier_semaphore()
    for to in ahead:
        pl.semaphore_signal(barrier, inc=1, device_id={"tp": to}, device_id_type=MESH)
    pl.semaphore_wait(barrier, len(RINGS))

    def block(r, back):
        cycle, way = RINGS[r]
        return device(cycle, pos[r] - way * back, k)

    own, whole = (dy, x), (gy, gx)

    def part(which, r, c, back):
        columns = pl.ds(pl.multiple_of(r * quarter + c * piece, piece), piece)
        return whole[which].at[at(block(r, back), rows), columns], columns

    def hop(which, r, c, step, first=False):
        to, columns = part(which, r, c, step)
        return pltpu.make_async_remote_copy(
            src_ref=own[which].at[:, columns] if first else to,
            dst_ref=to,
            send_sem=send.at[which, r, c, lax.rem(step, 2)],
            recv_sem=recv.at[which, r, c, step],
            device_id={"tp": ahead[r]},
            device_id_type=MESH,
        )

    def arrived(which, r, c, step):
        got, _ = part(which, r, c, step + 1)
        pltpu.make_async_remote_copy(
            src_ref=got, dst_ref=got, send_sem=send.at[which, r, c, 0],
            recv_sem=recv.at[which, r, c, step], device_id={"tp": ahead[r]}, device_id_type=MESH,
        ).wait_recv()

    def begin(which):
        for c in range(PIECES):
            for r in rings:
                hop(which, r, c, 0, True).start()

    def forward(which, step, c):
        for r in rings:
            arrived(which, r, c, step - 1)

            @pl.when(step >= 2)
            def _():
                hop(which, r, c, step - 2).wait_send()

            hop(which, r, c, step).start()

    def end(which):
        for c in range(PIECES):
            for r in rings:
                arrived(which, r, c, n - 2)
                hop(which, r, c, n - 3).wait_send()
                hop(which, r, c, n - 2).wait_send()

    begin(0)
    loads = [
        pltpu.make_async_copy(w_down.at[:, pl.ds(q * quarter, quarter)], w.at[pl.ds(q * ff, ff), :], w_sem.at[q])
        for q in rings
    ]
    for load in loads:
        load.start()
    for which in range(2):
        stage = wide.at[which, pl.ds(0, rows), :]
        pltpu.make_async_copy(own[which], stage, wide_sem.at[which]).start()
    for which in range(2):
        stage = wide.at[which, pl.ds(0, rows), :]
        pltpu.make_async_copy(own[which], stage, wide_sem.at[which]).wait()
        pltpu.make_async_copy(stage, whole[which].at[at(me, rows), :], wide_sem.at[which]).start()
    for which in range(2):
        stage = wide.at[which, pl.ds(0, rows), :]
        pltpu.make_async_copy(stage, whole[which].at[at(me, rows), :], wide_sem.at[which]).wait()
    for load in loads:
        load.wait()

    def gather_dy(step, _):
        for c in range(PIECES):
            forward(0, step, c)
        return 0

    lax.fori_loop(1, n - 1, gather_dy, 0)
    begin(1)
    end(0)

    chunks = tokens // CHUNK
    subs = ff // SUB

    def chunk_in(i):
        slot = lax.rem(i, 2)
        return (
            pltpu.make_async_copy(gy.at[at(i, CHUNK), :], wide.at[slot], wide_sem.at[slot]),
            pltpu.make_async_copy(pre.at[at(i, CHUNK), :], pre_in.at[slot], wide_sem.at[2 + slot]),
        )

    def tall_in(source, j):
        slot = lax.rem(j, 2)
        return pltpu.make_async_copy(source.at[:, at(j, SUB)], tall.at[slot], tall_sem.at[slot])

    for copy in chunk_in(0):
        copy.start()

    def chunk_step(i, _):
        slot = lax.rem(i, 2)
        for copy in chunk_in(i):
            copy.wait()

        @pl.when(i + 1 < chunks)
        def _():
            for copy in chunk_in(i + 1):
                copy.start()

        def sub_step(m, _):
            d_hidden = jnp.zeros((CHUNK, SUB), F32)
            for q in rings:
                d_hidden += lax.dot_general(
                    wide[slot, :, pl.ds(q * quarter, quarter)],
                    w[pl.ds(pl.multiple_of(q * ff + m * SUB, SUB), SUB), :],
                    NT, preferred_element_type=F32,
                )
            hidden, back = jax.vjp(act, pre_in[slot, :, at(m, SUB)].astype(F32))
            d_pre[at(i, CHUNK), at(m, SUB)] = back(d_hidden)[0].astype(BF16)
            turned[at(m, SUB), at(i, CHUNK)] = hidden.astype(BF16).T

            @pl.when(m == 1)
            def _():
                forward(1, i + 1, 0)

            @pl.when(m == subs - 1)
            def _():
                forward(1, i + 1, 1)

            return 0

        lax.fori_loop(0, subs, sub_step, 0)
        return 0

    tall_in(gy, 0).start()
    lax.fori_loop(0, chunks, chunk_step, 0)

    w_loads = [
        pltpu.make_async_copy(w_in.at[pl.ds(q * quarter, quarter), :], w.at[pl.ds(q * quarter, quarter), :], w_sem.at[q])
        for q in rings
    ]
    for load in w_loads:
        load.start()

    tiles = d // SUB

    def down_out(j):
        slot = lax.rem(j, 2)
        return pltpu.make_async_copy(out_a.at[slot], dw_down.at[:, at(j, SUB)], out_sem.at[slot])

    def down_tile(j):
        slot = lax.rem(j, 2)
        tall_in(gy, j).wait()

        @pl.when(j + 1 < tiles)
        def _():
            tall_in(gy, j + 1).start()

        @pl.when(j >= 2)
        def _():
            down_out(j - 2).wait()

        out_a[slot] = lax.dot_general(turned[...], tall[slot], NN, preferred_element_type=F32).astype(BF16)
        down_out(j).start()

    rest = n - 2 - chunks
    per = -(-tiles // rest)

    def down_step(t, _):
        def one(j, _):
            @pl.when(j < tiles)
            def _():
                down_tile(j)

            return 0

        forward(1, chunks + 1 + t, 0)
        lax.fori_loop(t * per, t * per + per // 2 + 1, one, 0)
        forward(1, chunks + 1 + t, 1)
        lax.fori_loop(t * per + per // 2 + 1, t * per + per, one, 0)
        return 0

    lax.fori_loop(0, rest, down_step, 0)
    down_out(tiles - 2).wait()
    down_out(tiles - 1).wait()
    for load in w_loads:
        load.wait()

    def term_of(r, step):
        return lax.dot_general(
            d_pre[at(block(r, step + 1), rows), :], w[pl.ds(r * quarter, quarter), :], NT, preferred_element_type=F32
        )

    def out_part(r, c, step):
        return wide.at[0, pl.ds(pl.multiple_of((lax.rem(step, 2) * PIECES + c) * half, half), half), pl.ds(r * quarter, quarter)]

    def in_part(r, c):
        return wide.at[1, pl.ds(pl.multiple_of(c * half, half), half), pl.ds(r * quarter, quarter)]

    def push(r, c, step):
        return pltpu.make_async_remote_copy(
            src_ref=out_part(r, c, step),
            dst_ref=land.at[r, step, pl.ds(pl.multiple_of(c * half, half), half), :],
            send_sem=rs_send.at[r, c, lax.rem(step, 2)],
            recv_sem=rs_recv.at[r, c, step],
            device_id={"tp": ahead[r]},
            device_id_type=MESH,
        )

    def fetch(r, c, step):
        return pltpu.make_async_copy(
            land.at[r, step, pl.ds(pl.multiple_of(c * half, half), half), :], in_part(r, c), fetch_sem.at[r, c]
        )

    def terms(step):
        for r in rings:
            term[r] = term_of(r, step)

    def sums(step, c, store):
        for r in rings:
            push(r, c, step - 1).wait_recv()
            fetch(r, c, step - 1).start()
        for r in rings:
            fetch(r, c, step - 1).wait()
            mine = term[r, pl.ds(pl.multiple_of(c * half, half), half), :]
            store(r, (in_part(r, c)[...].astype(F32) + mine).astype(BF16))

    def send_on(step, c):
        def store(r, value):
            @pl.when(step >= 2)
            def _():
                push(r, c, step - 2).wait_send()

            out_part(r, c, step)[...] = value
            if r >= 1:
                push(r - 1, c, step).start()

        sums(step, c, store)
        push(rings[-1], c, step).start()

    for r in rings:
        value = term_of(r, 0).astype(BF16)
        for c in range(PIECES):
            out_part(r, c, 0)[...] = value[c * half : (c + 1) * half]
        if r >= 1:
            for c in range(PIECES):
                push(r - 1, c, 0).start()
    for c in range(PIECES):
        push(rings[-1], c, 0).start()

    def turn(i, _):
        for m in range(subs):
            turned[pl.ds(m * SUB, SUB), at(i, CHUNK)] = d_pre[at(i, CHUNK), pl.ds(m * SUB, SUB)].T
        return 0

    lax.fori_loop(0, chunks, turn, 0)
    terms(1)
    end(1)
    tall_in(gx, 0).start()

    def in_out(j):
        slot = lax.rem(j, 2)
        return pltpu.make_async_copy(out_b.at[slot], dw_in.at[at(j, SUB), :], out_sem.at[2 + slot])

    def in_tile(j):
        slot = lax.rem(j, 2)
        tall_in(gx, j).wait()

        @pl.when(j + 1 < tiles)
        def _():
            tall_in(gx, j + 1).start()

        @pl.when(j >= 2)
        def _():
            in_out(j - 2).wait()

        product = lax.dot_general(turned[...], tall[slot], NN, preferred_element_type=F32)
        out_b[slot] = product.astype(BF16).T
        in_out(j).start()

    ticks = (n - 2) * PIECES

    def tick(t, _):
        step, c = 1 + t // PIECES, lax.rem(t, PIECES)
        send_on(step, c)

        @pl.when(c == PIECES - 1)
        def _():
            terms(step + 1)

        j = (t * tiles) // ticks

        @pl.when(((t + 1) * tiles) // ticks > j)
        def _():
            in_tile(j)

        return 0

    lax.fori_loop(0, ticks, tick, 0)

    for c in range(PIECES):
        def keep(r, value):
            push(r, c, n - 3).wait_send()
            out_part(r, c, n - 3)[...] = value

        sums(n - 1, c, keep)
        finished = wide.at[0, pl.ds((((n - 3) % 2) * PIECES + c) * half, half), :]
        pltpu.make_async_copy(finished, dx.at[pl.ds(c * half, half), :], w_sem.at[c]).start()
    for c in range(PIECES):
        finished = wide.at[0, pl.ds((((n - 3) % 2) * PIECES + c) * half, half), :]
        pltpu.make_async_copy(finished, dx.at[pl.ds(c * half, half), :], w_sem.at[c]).wait()
        for r in rings:
            push(r, c, n - 2).wait_send()
    in_out(tiles - 2).wait()
    in_out(tiles - 1).wait()


def solution(mesh):
    n = mesh.shape["tp"]

    def local(x, dy, pre, w_in, w_down):
        rows, d = x.shape
        tokens, ff = pre.shape
        quarter = d // len(RINGS)
        hbm = pl.BlockSpec(memory_space=pl.ANY)
        outs = [
            (rows, d), (d, ff), (ff, d), (tokens, d), (tokens, d), (len(RINGS), n - 1, rows, quarter),
        ]
        outs = [jax.ShapeDtypeStruct(s, BF16) for s in outs]
        dma = pltpu.SemaphoreType.DMA
        flops = 8 * tokens * d * ff
        return pl.pallas_call(
            functools.partial(kernel, n),
            out_shape=outs,
            in_specs=[hbm] * 5,
            out_specs=[hbm] * len(outs),
            scratch_shapes=[
                pltpu.VMEM((d, ff), BF16),
                pltpu.VMEM((tokens, ff), BF16),
                pltpu.VMEM((ff, tokens), BF16),
                pltpu.VMEM((2, CHUNK, d), BF16),
                pltpu.VMEM((2, CHUNK, ff), BF16),
                pltpu.VMEM((2, tokens, SUB), BF16),
                pltpu.VMEM((2, ff, SUB), BF16),
                pltpu.VMEM((2, SUB, ff), BF16),
                pltpu.VMEM((len(RINGS), rows, quarter), F32),
                dma((2, len(RINGS), PIECES, 2)),
                dma((2, len(RINGS), PIECES, n - 1)),
                dma((len(RINGS), PIECES, 2)),
                dma((len(RINGS), PIECES, n - 1)),
                dma((len(RINGS),)),
                dma((4,)),
                dma((2,)),
                dma((4,)),
                dma((len(RINGS), PIECES)),
            ],
            compiler_params=pltpu.CompilerParams(
                collective_id=0, has_side_effects=True, vmem_limit_bytes=67_043_328
            ),
            cost_estimate=pl.CostEstimate(flops=flops, bytes_accessed=10 * tokens * d, transcendentals=tokens * ff),
            name="mlp_backward",
        )(x, dy, pre, w_in, w_down)[:3]

    rows = P(("dp", "tp"), None)
    return jax.shard_map(
        local,
        mesh=mesh,
        in_specs=(rows, rows, P("dp", "tp"), P(None, "tp"), P("tp", None)),
        out_specs=(rows, P("dp", "tp"), rows),
        check_vma=False,
    )
```

```python
import functools
import math

import jax
import jax.numpy as jnp
from jax import lax
from jax.experimental import pallas as pl
from jax.experimental.pallas import tpu as pltpu

P = jax.sharding.PartitionSpec
MESH = pl.DeviceIdType.MESH
F32, BF16 = jnp.float32, jnp.bfloat16
RINGS = ((0, 1), (0, -1), (1, 1), (1, -1))
PIECES = 2
CHUNK = 512
SUB = 256


def act(pre):
    return jax.nn.gelu(pre)


def position(cycle, me, k):
    x, y = me // k, lax.rem(me, k)
    return (x if cycle == 0 else y) * k + lax.rem(x + y, k)


def device(cycle, pos, k):
    n = k * k
    rem = (lambda a, b: a % b) if isinstance(pos, int) else lax.rem
    pos = rem(pos + 4 * n, n)
    a, b = pos // k, rem(pos, k)
    m = rem(b - a + k, k)
    return a * k + m if cycle == 0 else m * k + a


def at(i, size):
    return pl.ds(pl.multiple_of(i * size, size), size)


NT = (((1,), (1,)), ((), ()))
NN = (((1,), (0,)), ((), ()))


def kernel(
    n, x, dy, pre, w_in, w_down, dw_in, dw_down, own_term, last_0, last_1, last_2, last_3, gx, gy, land,
    w, d_pre, turned, wide, pre_in, tall, out_a, out_b, term,
    send, recv, rs_send, rs_recv, w_sem, wide_sem, tall_sem, out_sem, fetch_sem, own_sem,
):
    k = math.isqrt(n)
    rows, d = x.shape
    tokens, ff = d_pre.shape
    quarter = d // len(RINGS)
    piece = quarter // PIECES
    half = rows // PIECES
    rings = range(len(RINGS))
    me = lax.axis_index("tp")
    pos = [position(cycle, me, k) for cycle, _ in RINGS]
    ahead = [device(c, pos[r] + way, k) for r, (c, way) in enumerate(RINGS)]

    barrier = pltpu.get_barrier_semaphore()
    for to in ahead:
        pl.semaphore_signal(barrier, inc=1, device_id={"tp": to}, device_id_type=MESH)
    pl.semaphore_wait(barrier, len(RINGS))

    def block(r, back):
        cycle, way = RINGS[r]
        return device(cycle, pos[r] - way * back, k)

    own, whole = (dy, x), (gy, gx)

    def part(which, r, c, back):
        columns = pl.ds(pl.multiple_of(r * quarter + c * piece, piece), piece)
        return whole[which].at[at(block(r, back), rows), columns], columns

    def hop(which, r, c, step, first=False):
        to, columns = part(which, r, c, step)
        return pltpu.make_async_remote_copy(
            src_ref=own[which].at[:, columns] if first else to,
            dst_ref=to,
            send_sem=send.at[which, r, c, lax.rem(step, 2)],
            recv_sem=recv.at[which, r, c, step],
            device_id={"tp": ahead[r]},
            device_id_type=MESH,
        )

    def arrived(which, r, c, step):
        got, _ = part(which, r, c, step + 1)
        pltpu.make_async_remote_copy(
            src_ref=got, dst_ref=got, send_sem=send.at[which, r, c, 0],
            recv_sem=recv.at[which, r, c, step], device_id={"tp": ahead[r]}, device_id_type=MESH,
        ).wait_recv()

    def begin(which):
        for c in range(PIECES):
            for r in rings:
                hop(which, r, c, 0, True).start()

    def forward(which, step, c):
        for r in rings:
            arrived(which, r, c, step - 1)

            @pl.when(step >= 2)
            def _():
                hop(which, r, c, step - 2).wait_send()

            hop(which, r, c, step).start()

    def end(which):
        for c in range(PIECES):
            for r in rings:
                arrived(which, r, c, n - 2)
                hop(which, r, c, n - 3).wait_send()
                hop(which, r, c, n - 2).wait_send()

    begin(0)
    loads = [
        pltpu.make_async_copy(w_down.at[:, pl.ds(q * quarter, quarter)], w.at[pl.ds(q * ff, ff), :], w_sem.at[q])
        for q in rings
    ]
    for load in loads:
        load.start()
    for which in range(2):
        stage = wide.at[which, pl.ds(0, rows), :]
        pltpu.make_async_copy(own[which], stage, wide_sem.at[which]).start()
    for which in range(2):
        stage = wide.at[which, pl.ds(0, rows), :]
        pltpu.make_async_copy(own[which], stage, wide_sem.at[which]).wait()
        pltpu.make_async_copy(stage, whole[which].at[at(me, rows), :], wide_sem.at[which]).start()
    for which in range(2):
        stage = wide.at[which, pl.ds(0, rows), :]
        pltpu.make_async_copy(stage, whole[which].at[at(me, rows), :], wide_sem.at[which]).wait()
    for load in loads:
        load.wait()

    def gather_dy(step, _):
        for c in range(PIECES):
            forward(0, step, c)
        return 0

    lax.fori_loop(1, n - 1, gather_dy, 0)
    begin(1)
    end(0)

    chunks = tokens // CHUNK
    subs = ff // SUB

    def chunk_in(i):
        slot = lax.rem(i, 2)
        return (
            pltpu.make_async_copy(gy.at[at(i, CHUNK), :], wide.at[slot], wide_sem.at[slot]),
            pltpu.make_async_copy(pre.at[at(i, CHUNK), :], pre_in.at[slot], wide_sem.at[2 + slot]),
        )

    def tall_in(source, j):
        slot = lax.rem(j, 2)
        return pltpu.make_async_copy(source.at[:, at(j, SUB)], tall.at[slot], tall_sem.at[slot])

    for copy in chunk_in(0):
        copy.start()

    def chunk_step(i, _):
        slot = lax.rem(i, 2)
        for copy in chunk_in(i):
            copy.wait()

        @pl.when(i + 1 < chunks)
        def _():
            for copy in chunk_in(i + 1):
                copy.start()

        def sub_step(m, _):
            d_hidden = jnp.zeros((CHUNK, SUB), F32)
            for q in rings:
                d_hidden += lax.dot_general(
                    wide[slot, :, pl.ds(q * quarter, quarter)],
                    w[pl.ds(pl.multiple_of(q * ff + m * SUB, SUB), SUB), :],
                    NT, preferred_element_type=F32,
                )
            hidden, back = jax.vjp(act, pre_in[slot, :, at(m, SUB)].astype(F32))
            d_pre[at(i, CHUNK), at(m, SUB)] = back(d_hidden)[0].astype(BF16)
            turned[at(m, SUB), at(i, CHUNK)] = hidden.astype(BF16).T

            @pl.when(m == 1)
            def _():
                forward(1, i + 1, 0)

            @pl.when(m == subs - 1)
            def _():
                forward(1, i + 1, 1)

            return 0

        lax.fori_loop(0, subs, sub_step, 0)
        return 0

    tall_in(gy, 0).start()
    lax.fori_loop(0, chunks, chunk_step, 0)

    w_loads = [
        pltpu.make_async_copy(w_in.at[pl.ds(q * quarter, quarter), :], w.at[pl.ds(q * quarter, quarter), :], w_sem.at[q])
        for q in rings
    ]
    for load in w_loads:
        load.start()

    tiles = d // SUB

    def term_of(r, step):
        return lax.dot_general(
            d_pre[at(block(r, step + 1), rows), :], w[pl.ds(r * quarter, quarter), :], NT, preferred_element_type=F32
        )

    def terms(step):
        for r in rings:
            term[r] = term_of(r, step)

    own_copy = pltpu.make_async_copy(term, own_term, own_sem)

    def down_out(j):
        slot = lax.rem(j, 2)
        return pltpu.make_async_copy(out_a.at[slot], dw_down.at[:, at(j, SUB)], out_sem.at[slot])

    def down_tile(j):
        slot = lax.rem(j, 2)
        tall_in(gy, j).wait()

        @pl.when(j + 1 < tiles)
        def _():
            tall_in(gy, j + 1).start()

        @pl.when(j >= 2)
        def _():
            down_out(j - 2).wait()

        out_a[slot] = lax.dot_general(turned[...], tall[slot], NN, preferred_element_type=F32).astype(BF16)
        down_out(j).start()

    rest = n - 2 - chunks
    per = -(-tiles // rest)

    def down_step(t, _):
        def one(j, _):
            @pl.when(j < tiles)
            def _():
                down_tile(j)

            return 0

        forward(1, chunks + 1 + t, 0)
        lax.fori_loop(t * per, t * per + per // 2 + 1, one, 0)
        forward(1, chunks + 1 + t, 1)
        lax.fori_loop(t * per + per // 2 + 1, t * per + per, one, 0)

        @pl.when(t == rest // 2)
        def _():
            for load in w_loads:
                load.wait()
            terms(n - 1)
            own_copy.start()

        return 0

    lax.fori_loop(0, rest, down_step, 0)
    down_out(tiles - 2).wait()
    down_out(tiles - 1).wait()
    own_copy.wait()

    def out_part(r, c, step):
        return wide.at[0, pl.ds(pl.multiple_of((lax.rem(step, 2) * PIECES + c) * half, half), half), pl.ds(r * quarter, quarter)]

    def in_part(r, c):
        return wide.at[1, pl.ds(pl.multiple_of(c * half, half), half), pl.ds(r * quarter, quarter)]

    def push(r, c, step):
        return pltpu.make_async_remote_copy(
            src_ref=out_part(r, c, step),
            dst_ref=land.at[r, step, pl.ds(pl.multiple_of(c * half, half), half), :],
            send_sem=rs_send.at[r, c, lax.rem(step, 2)],
            recv_sem=rs_recv.at[r, c, step],
            device_id={"tp": ahead[r]},
            device_id_type=MESH,
        )

    def fetch(r, c, step):
        return pltpu.make_async_copy(
            land.at[r, step, pl.ds(pl.multiple_of(c * half, half), half), :], in_part(r, c), fetch_sem.at[r, c]
        )

    def sums(step, c, store):
        for r in rings:
            push(r, c, step - 1).wait_recv()
            fetch(r, c, step - 1).start()
        for r in rings:
            fetch(r, c, step - 1).wait()
            mine = term[r, pl.ds(pl.multiple_of(c * half, half), half), :]
            store(r, (in_part(r, c)[...].astype(F32) + mine).astype(BF16))

    def send_on(step, c):
        def store(r, value):
            @pl.when(step >= 2)
            def _():
                push(r, c, step - 2).wait_send()

            out_part(r, c, step)[...] = value
            if r >= 1:
                push(r - 1, c, step).start()

        sums(step, c, store)
        push(rings[-1], c, step).start()

    for r in rings:
        value = term_of(r, 0).astype(BF16)
        for c in range(PIECES):
            out_part(r, c, 0)[...] = value[c * half : (c + 1) * half]
        if r >= 1:
            for c in range(PIECES):
                push(r - 1, c, 0).start()
    for c in range(PIECES):
        push(rings[-1], c, 0).start()

    def turn(i, _):
        for m in range(subs):
            turned[pl.ds(m * SUB, SUB), at(i, CHUNK)] = d_pre[at(i, CHUNK), pl.ds(m * SUB, SUB)].T
        return 0

    lax.fori_loop(0, chunks, turn, 0)
    terms(1)
    end(1)
    tall_in(gx, 0).start()

    def in_out(j):
        slot = lax.rem(j, 2)
        return pltpu.make_async_copy(out_b.at[slot], dw_in.at[at(j, SUB), :], out_sem.at[2 + slot])

    def in_tile(j):
        slot = lax.rem(j, 2)
        tall_in(gx, j).wait()

        @pl.when(j + 1 < tiles)
        def _():
            tall_in(gx, j + 1).start()

        @pl.when(j >= 2)
        def _():
            in_out(j - 2).wait()

        product = lax.dot_general(turned[...], tall[slot], NN, preferred_element_type=F32)
        out_b[slot] = product.astype(BF16).T
        in_out(j).start()

    ticks = (n - 3) * PIECES

    def tick(t, _):
        step, c = 1 + t // PIECES, lax.rem(t, PIECES)
        send_on(step, c)

        @pl.when(c == PIECES - 1)
        def _():
            terms(step + 1)

        j = (t * tiles) // ticks

        @pl.when(((t + 1) * tiles) // ticks > j)
        def _():
            in_tile(j)

        return 0

    lax.fori_loop(0, ticks, tick, 0)

    last = (last_0, last_1, last_2, last_3)

    def hand_over(r, c):
        return pltpu.make_async_copy(out_part(r, c, n - 2), last[r].at[pl.ds(c * half, half), :], fetch_sem.at[r, c])

    for c in range(PIECES):
        def keep(r, value):
            push(r, c, n - 4).wait_send()
            out_part(r, c, n - 2)[...] = value
            if r >= 1:
                hand_over(r - 1, c).start()

        sums(n - 2, c, keep)
        hand_over(rings[-1], c).start()
    for c in range(PIECES):
        for r in rings:
            hand_over(r, c).wait()
            push(r, c, n - 3).wait_send()
    in_out(tiles - 2).wait()
    in_out(tiles - 1).wait()


def settle(*arrays):
    def body(*refs):
        for i in range(len(arrays)):
            refs[len(arrays) + i][...] = refs[i][...]

    steps = 10
    specs = [pl.BlockSpec((a.shape[0] // steps, a.shape[1]), lambda i: (i, 0)) for a in arrays]
    size = sum(a.size for a in arrays)
    return pl.pallas_call(
        body,
        grid=(steps,),
        out_shape=[jax.ShapeDtypeStruct(a.shape, a.dtype) for a in arrays],
        in_specs=specs,
        out_specs=specs,
        cost_estimate=pl.CostEstimate(flops=2000 * size, bytes_accessed=4 * size, transcendentals=0),
        name="settle",
    )(*arrays)


def finish(own_term, *came):
    rows, quarter = came[0].shape
    steps = 2

    def body(own, *refs):
        out = refs[-1]
        for r, got in enumerate(refs[:-1]):
            out[:, pl.ds(r * quarter, quarter)] = (got[...].astype(F32) + own[r]).astype(BF16)

    return pl.pallas_call(
        body,
        grid=(steps,),
        out_shape=jax.ShapeDtypeStruct((rows, quarter * len(came)), BF16),
        in_specs=[pl.BlockSpec((len(came), rows // steps, quarter), lambda i: (0, i, 0))]
        + [pl.BlockSpec((rows // steps, quarter), lambda i: (i, 0))] * len(came),
        out_specs=pl.BlockSpec((rows // steps, quarter * len(came)), lambda i: (i, 0)),
        name="finish",
    )(own_term, *came)


def solution(mesh):
    n = mesh.shape["tp"]
    k = math.isqrt(n)

    def local(x, dy, pre, w_in, w_down):
        rows, d = x.shape
        tokens, ff = pre.shape
        quarter = d // len(RINGS)
        hbm = pl.BlockSpec(memory_space=pl.ANY)
        outs = [
            (d, ff), (ff, d), *[(rows, quarter)] * len(RINGS), (tokens, d), (tokens, d),
            (len(RINGS), n - 2, rows, quarter),
        ]
        outs = [jax.ShapeDtypeStruct(s, BF16) for s in outs]
        outs.insert(2, jax.ShapeDtypeStruct((len(RINGS), rows, quarter), F32))
        dma = pltpu.SemaphoreType.DMA
        flops = 8 * tokens * d * ff
        dw_in, dw_down, own_term, *last = pl.pallas_call(
            functools.partial(kernel, n),
            out_shape=outs,
            in_specs=[hbm] * 5,
            out_specs=[hbm] * len(outs),
            scratch_shapes=[
                pltpu.VMEM((d, ff), BF16),
                pltpu.VMEM((tokens, ff), BF16),
                pltpu.VMEM((ff, tokens), BF16),
                pltpu.VMEM((2, CHUNK, d), BF16),
                pltpu.VMEM((2, CHUNK, ff), BF16),
                pltpu.VMEM((2, tokens, SUB), BF16),
                pltpu.VMEM((2, ff, SUB), BF16),
                pltpu.VMEM((2, SUB, ff), BF16),
                pltpu.VMEM((len(RINGS), rows, quarter), F32),
                dma((2, len(RINGS), PIECES, 2)),
                dma((2, len(RINGS), PIECES, n - 1)),
                dma((len(RINGS), PIECES, 2)),
                dma((len(RINGS), PIECES, n - 2)),
                dma((len(RINGS),)),
                dma((4,)),
                dma((2,)),
                dma((4,)),
                dma((len(RINGS), PIECES)),
                dma(()),
            ],
            compiler_params=pltpu.CompilerParams(
                collective_id=0, has_side_effects=True, vmem_limit_bytes=67_043_328
            ),
            cost_estimate=pl.CostEstimate(flops=flops, bytes_accessed=10 * tokens * d, transcendentals=tokens * ff),
            name="mlp_backward",
        )(x, dy, pre, w_in, w_down)
        last = last[: len(RINGS)]
        hops = [[(device(c, i, k), device(c, i + way, k)) for i in range(n)] for c, way in RINGS]
        came = [lax.ppermute(t, "tp", hop) for t, hop in zip(last, hops)]
        dw_in, dw_down = settle(dw_in, dw_down)
        return finish(own_term, *came), dw_in, dw_down

    rows = P(("dp", "tp"), None)
    return jax.shard_map(
        local,
        mesh=mesh,
        in_specs=(rows, rows, P("dp", "tp"), P(None, "tp"), P("tp", None)),
        out_specs=(rows, P("dp", "tp"), rows),
        check_vma=False,
    )
```

```python
import functools
import math

import jax
import jax.numpy as jnp
from jax import lax
from jax.experimental import pallas as pl
from jax.experimental.pallas import tpu as pltpu

P = jax.sharding.PartitionSpec
MESH = pl.DeviceIdType.MESH
F32, BF16 = jnp.float32, jnp.bfloat16
RINGS = ((0, 1), (0, -1), (1, 1), (1, -1))
PIECES = 2
CHUNK = 512
SUB = 256


def act(pre):
    return jax.nn.gelu(pre)


def position(cycle, me, k):
    x, y = me // k, lax.rem(me, k)
    return (x if cycle == 0 else y) * k + lax.rem(x + y, k)


def device(cycle, pos, k):
    n = k * k
    rem = (lambda a, b: a % b) if isinstance(pos, int) else lax.rem
    pos = rem(pos + 4 * n, n)
    a, b = pos // k, rem(pos, k)
    m = rem(b - a + k, k)
    return a * k + m if cycle == 0 else m * k + a


def at(i, size):
    return pl.ds(pl.multiple_of(i * size, size), size)


NT = (((1,), (1,)), ((), ()))
NN = (((1,), (0,)), ((), ()))


def kernel(
    n, x, dy, pre, w_in, w_down, dw_in, dw_down, own_term, last_0, last_1, last_2, last_3, gx, gy, land,
    w, d_pre, turned, wide, pre_in, tall, out_a, out_b, term,
    send, recv, rs_send, rs_recv, w_sem, wide_sem, tall_sem, out_sem, fetch_sem, own_sem,
):
    k = math.isqrt(n)
    rows, d = x.shape
    tokens, ff = d_pre.shape
    quarter = d // len(RINGS)
    piece = quarter // PIECES
    half = rows // PIECES
    rings = range(len(RINGS))
    me = lax.axis_index("tp")
    pos = [position(cycle, me, k) for cycle, _ in RINGS]
    ahead = [device(c, pos[r] + way, k) for r, (c, way) in enumerate(RINGS)]

    barrier = pltpu.get_barrier_semaphore()
    for to in ahead:
        pl.semaphore_signal(barrier, inc=1, device_id={"tp": to}, device_id_type=MESH)
    pl.semaphore_wait(barrier, len(RINGS))

    def block(r, back):
        cycle, way = RINGS[r]
        return device(cycle, pos[r] - way * back, k)

    own, whole = (dy, x), (gy, gx)

    def part(which, r, c, back):
        columns = pl.ds(pl.multiple_of(r * quarter + c * piece, piece), piece)
        return whole[which].at[at(block(r, back), rows), columns], columns

    def hop(which, r, c, step, first=False):
        to, columns = part(which, r, c, step)
        return pltpu.make_async_remote_copy(
            src_ref=own[which].at[:, columns] if first else to,
            dst_ref=to,
            send_sem=send.at[which, r, c, lax.rem(step, 2)],
            recv_sem=recv.at[which, r, c, step],
            device_id={"tp": ahead[r]},
            device_id_type=MESH,
        )

    def arrived(which, r, c, step):
        got, _ = part(which, r, c, step + 1)
        pltpu.make_async_remote_copy(
            src_ref=got, dst_ref=got, send_sem=send.at[which, r, c, 0],
            recv_sem=recv.at[which, r, c, step], device_id={"tp": ahead[r]}, device_id_type=MESH,
        ).wait_recv()

    def begin(which):
        for c in range(PIECES):
            for r in rings:
                hop(which, r, c, 0, True).start()

    def forward(which, step, c):
        for r in rings:
            arrived(which, r, c, step - 1)

            @pl.when(step >= 2)
            def _():
                hop(which, r, c, step - 2).wait_send()

            hop(which, r, c, step).start()

    def end(which):
        for c in range(PIECES):
            for r in rings:
                arrived(which, r, c, n - 2)
                hop(which, r, c, n - 3).wait_send()
                hop(which, r, c, n - 2).wait_send()

    begin(0)
    loads = [
        pltpu.make_async_copy(w_down.at[:, pl.ds(q * quarter, quarter)], w.at[pl.ds(q * ff, ff), :], w_sem.at[q])
        for q in rings
    ]
    for load in loads:
        load.start()
    for which in range(2):
        stage = wide.at[which, pl.ds(0, rows), :]
        pltpu.make_async_copy(own[which], stage, wide_sem.at[which]).start()
    for which in range(2):
        stage = wide.at[which, pl.ds(0, rows), :]
        pltpu.make_async_copy(own[which], stage, wide_sem.at[which]).wait()
        pltpu.make_async_copy(stage, whole[which].at[at(me, rows), :], wide_sem.at[which]).start()
    for which in range(2):
        stage = wide.at[which, pl.ds(0, rows), :]
        pltpu.make_async_copy(stage, whole[which].at[at(me, rows), :], wide_sem.at[which]).wait()
    for load in loads:
        load.wait()

    def gather_dy(step, _):
        for c in range(PIECES):
            forward(0, step, c)
        return 0

    lax.fori_loop(1, n - 1, gather_dy, 0)
    begin(1)
    end(0)

    chunks = tokens // CHUNK
    subs = ff // SUB

    def chunk_in(i):
        slot = lax.rem(i, 2)
        return (
            pltpu.make_async_copy(gy.at[at(i, CHUNK), :], wide.at[slot], wide_sem.at[slot]),
            pltpu.make_async_copy(pre.at[at(i, CHUNK), :], pre_in.at[slot], wide_sem.at[2 + slot]),
        )

    def tall_in(source, j):
        slot = lax.rem(j, 2)
        return pltpu.make_async_copy(source.at[:, at(j, SUB)], tall.at[slot], tall_sem.at[slot])

    for copy in chunk_in(0):
        copy.start()

    def chunk_step(i, _):
        slot = lax.rem(i, 2)
        for copy in chunk_in(i):
            copy.wait()

        @pl.when(i + 1 < chunks)
        def _():
            for copy in chunk_in(i + 1):
                copy.start()

        def sub_step(m, _):
            d_hidden = jnp.zeros((CHUNK, SUB), F32)
            for q in rings:
                d_hidden += lax.dot_general(
                    wide[slot, :, pl.ds(q * quarter, quarter)],
                    w[pl.ds(pl.multiple_of(q * ff + m * SUB, SUB), SUB), :],
                    NT, preferred_element_type=F32,
                )
            hidden, back = jax.vjp(act, pre_in[slot, :, at(m, SUB)].astype(F32))
            d_pre[at(i, CHUNK), at(m, SUB)] = back(d_hidden)[0].astype(BF16)
            turned[at(m, SUB), at(i, CHUNK)] = hidden.astype(BF16).T

            @pl.when(m == 1)
            def _():
                forward(1, i + 1, 0)

            @pl.when(m == subs - 1)
            def _():
                forward(1, i + 1, 1)

            return 0

        lax.fori_loop(0, subs, sub_step, 0)
        return 0

    tall_in(gy, 0).start()
    lax.fori_loop(0, chunks, chunk_step, 0)

    w_loads = [
        pltpu.make_async_copy(w_in.at[pl.ds(q * quarter, quarter), :], w.at[pl.ds(q * quarter, quarter), :], w_sem.at[q])
        for q in rings
    ]
    for load in w_loads:
        load.start()

    tiles = d // SUB

    def term_of(r, step):
        return lax.dot_general(
            d_pre[at(block(r, step + 1), rows), :], w[pl.ds(r * quarter, quarter), :], NT, preferred_element_type=F32
        )

    def terms(step):
        for r in rings:
            term[r] = term_of(r, step)

    own_copy = pltpu.make_async_copy(term, own_term, own_sem)

    def down_out(j):
        slot = lax.rem(j, 2)
        return pltpu.make_async_copy(out_a.at[slot], dw_down.at[:, at(j, SUB)], out_sem.at[slot])

    def down_tile(j):
        slot = lax.rem(j, 2)
        tall_in(gy, j).wait()

        @pl.when(j + 1 < tiles)
        def _():
            tall_in(gy, j + 1).start()

        @pl.when(j >= 2)
        def _():
            down_out(j - 2).wait()

        out_a[slot] = lax.dot_general(turned[...], tall[slot], NN, preferred_element_type=F32).astype(BF16)
        down_out(j).start()

    rest = n - 2 - chunks
    per = -(-tiles // rest)

    def down_step(t, _):
        def one(j, _):
            @pl.when(j < tiles)
            def _():
                down_tile(j)

            return 0

        forward(1, chunks + 1 + t, 0)
        lax.fori_loop(t * per, t * per + per // 2 + 1, one, 0)
        forward(1, chunks + 1 + t, 1)
        lax.fori_loop(t * per + per // 2 + 1, t * per + per, one, 0)

        @pl.when(t == rest // 2)
        def _():
            for load in w_loads:
                load.wait()
            terms(n - 1)
            own_copy.start()

        return 0

    lax.fori_loop(0, rest, down_step, 0)
    down_out(tiles - 2).wait()
    down_out(tiles - 1).wait()
    own_copy.wait()

    def out_part(r, c, step):
        return wide.at[0, pl.ds(pl.multiple_of((lax.rem(step, 2) * PIECES + c) * half, half), half), pl.ds(r * quarter, quarter)]

    def in_part(r, c):
        return wide.at[1, pl.ds(pl.multiple_of(c * half, half), half), pl.ds(r * quarter, quarter)]

    def push(r, c, step):
        return pltpu.make_async_remote_copy(
            src_ref=out_part(r, c, step),
            dst_ref=land.at[r, step, pl.ds(pl.multiple_of(c * half, half), half), :],
            send_sem=rs_send.at[r, c, lax.rem(step, 2)],
            recv_sem=rs_recv.at[r, c, step],
            device_id={"tp": ahead[r]},
            device_id_type=MESH,
        )

    def fetch(r, c, step):
        return pltpu.make_async_copy(
            land.at[r, step, pl.ds(pl.multiple_of(c * half, half), half), :], in_part(r, c), fetch_sem.at[r, c]
        )

    def sums(step, c, store):
        for r in rings:
            push(r, c, step - 1).wait_recv()
            fetch(r, c, step - 1).start()
        for r in rings:
            fetch(r, c, step - 1).wait()
            mine = term[r, pl.ds(pl.multiple_of(c * half, half), half), :]
            store(r, (in_part(r, c)[...].astype(F32) + mine).astype(BF16))

    def send_on(step, c):
        def store(r, value):
            @pl.when(step >= 2)
            def _():
                push(r, c, step - 2).wait_send()

            out_part(r, c, step)[...] = value
            if r >= 1:
                push(r - 1, c, step).start()

        sums(step, c, store)
        push(rings[-1], c, step).start()

    for r in rings:
        value = term_of(r, 0).astype(BF16)
        for c in range(PIECES):
            out_part(r, c, 0)[...] = value[c * half : (c + 1) * half]
        if r >= 1:
            for c in range(PIECES):
                push(r - 1, c, 0).start()
    for c in range(PIECES):
        push(rings[-1], c, 0).start()

    def turn(i, _):
        for m in range(subs):
            turned[pl.ds(m * SUB, SUB), at(i, CHUNK)] = d_pre[at(i, CHUNK), pl.ds(m * SUB, SUB)].T
        return 0

    lax.fori_loop(0, chunks, turn, 0)
    terms(1)
    end(1)
    tall_in(gx, 0).start()

    def in_out(j):
        slot = lax.rem(j, 2)
        return pltpu.make_async_copy(out_b.at[slot], dw_in.at[at(j, SUB), :], out_sem.at[2 + slot])

    def in_tile(j):
        slot = lax.rem(j, 2)
        tall_in(gx, j).wait()

        @pl.when(j + 1 < tiles)
        def _():
            tall_in(gx, j + 1).start()

        @pl.when(j >= 2)
        def _():
            in_out(j - 2).wait()

        product = lax.dot_general(turned[...], tall[slot], NN, preferred_element_type=F32)
        out_b[slot] = product.astype(BF16).T
        in_out(j).start()

    ticks = (n - 3) * PIECES

    def tick(t, _):
        step, c = 1 + t // PIECES, lax.rem(t, PIECES)
        send_on(step, c)

        @pl.when(c == PIECES - 1)
        def _():
            terms(step + 1)

        j = (t * tiles) // ticks

        @pl.when(((t + 1) * tiles) // ticks > j)
        def _():
            in_tile(j)

        return 0

    lax.fori_loop(0, ticks, tick, 0)

    last = (last_0, last_1, last_2, last_3)

    def hand_over(r, c):
        return pltpu.make_async_copy(out_part(r, c, n - 2), last[r].at[pl.ds(c * half, half), :], fetch_sem.at[r, c])

    for c in range(PIECES):
        def keep(r, value):
            push(r, c, n - 4).wait_send()
            out_part(r, c, n - 2)[...] = value
            if r >= 1:
                hand_over(r - 1, c).start()

        sums(n - 2, c, keep)
        hand_over(rings[-1], c).start()
    for c in range(PIECES):
        for r in rings:
            hand_over(r, c).wait()
            push(r, c, n - 3).wait_send()
    in_out(tiles - 2).wait()
    in_out(tiles - 1).wait()


def settle(*arrays):
    steps = 8
    count = len(arrays)

    def body(*refs):
        sources, targets, stages = (refs[i * count : (i + 1) * count] for i in range(3))
        sems = refs[3 * count]
        pairs = [(i, step) for step in range(steps) for i in range(count)]

        def rows(i, step):
            height = arrays[i].shape[0] // steps
            return pl.ds(step * height, height)

        def read(i, step):
            return pltpu.make_async_copy(sources[i].at[rows(i, step), :], stages[i].at[step], sems.at[0, i, step])

        def write(i, step):
            return pltpu.make_async_copy(stages[i].at[step], targets[i].at[rows(i, step), :], sems.at[1, i, step])

        for pair in pairs:
            read(*pair).start()
        for pair in pairs:
            read(*pair).wait()
            write(*pair).start()
        for pair in pairs:
            write(*pair).wait()

    size = sum(a.size for a in arrays)
    hbm = pl.BlockSpec(memory_space=pl.ANY)
    return pl.pallas_call(
        body,
        out_shape=[jax.ShapeDtypeStruct(a.shape, a.dtype) for a in arrays],
        in_specs=[hbm] * count,
        out_specs=[hbm] * count,
        scratch_shapes=[pltpu.VMEM((steps, a.shape[0] // steps, a.shape[1]), a.dtype) for a in arrays]
        + [pltpu.SemaphoreType.DMA((2, count, steps))],
        compiler_params=pltpu.CompilerParams(vmem_limit_bytes=54 * 2**20),
        cost_estimate=pl.CostEstimate(flops=2000 * size, bytes_accessed=4 * size, transcendentals=0),
        name="settle",
    )(*arrays)


def finish(own_term, *came):
    rows, quarter = came[0].shape

    def body(own, *refs):
        out = refs[-1]
        for r, got in enumerate(refs[:-1]):
            out[:, pl.ds(r * quarter, quarter)] = (got[...].astype(F32) + own[r]).astype(BF16)

    vmem = pl.BlockSpec(memory_space=pltpu.VMEM)
    return pl.pallas_call(
        body,
        out_shape=jax.ShapeDtypeStruct((rows, quarter * len(came)), BF16),
        in_specs=[vmem] * (1 + len(came)),
        out_specs=vmem,
        compiler_params=pltpu.CompilerParams(vmem_limit_bytes=16 * 2**20),
        name="finish",
    )(own_term, *came)


def solution(mesh):
    n = mesh.shape["tp"]
    k = math.isqrt(n)

    def local(x, dy, pre, w_in, w_down):
        rows, d = x.shape
        tokens, ff = pre.shape
        quarter = d // len(RINGS)
        hbm = pl.BlockSpec(memory_space=pl.ANY)
        outs = [
            (d, ff), (ff, d), *[(rows, quarter)] * len(RINGS), (tokens, d), (tokens, d),
            (len(RINGS), n - 2, rows, quarter),
        ]
        outs = [jax.ShapeDtypeStruct(s, BF16) for s in outs]
        outs.insert(2, jax.ShapeDtypeStruct((len(RINGS), rows, quarter), F32))
        dma = pltpu.SemaphoreType.DMA
        flops = 8 * tokens * d * ff
        dw_in, dw_down, own_term, *last = pl.pallas_call(
            functools.partial(kernel, n),
            out_shape=outs,
            in_specs=[hbm] * 5,
            out_specs=[hbm] * len(outs),
            scratch_shapes=[
                pltpu.VMEM((d, ff), BF16),
                pltpu.VMEM((tokens, ff), BF16),
                pltpu.VMEM((ff, tokens), BF16),
                pltpu.VMEM((2, CHUNK, d), BF16),
                pltpu.VMEM((2, CHUNK, ff), BF16),
                pltpu.VMEM((2, tokens, SUB), BF16),
                pltpu.VMEM((2, ff, SUB), BF16),
                pltpu.VMEM((2, SUB, ff), BF16),
                pltpu.VMEM((len(RINGS), rows, quarter), F32),
                dma((2, len(RINGS), PIECES, 2)),
                dma((2, len(RINGS), PIECES, n - 1)),
                dma((len(RINGS), PIECES, 2)),
                dma((len(RINGS), PIECES, n - 2)),
                dma((len(RINGS),)),
                dma((4,)),
                dma((2,)),
                dma((4,)),
                dma((len(RINGS), PIECES)),
                dma(()),
            ],
            compiler_params=pltpu.CompilerParams(
                collective_id=0, has_side_effects=True, vmem_limit_bytes=67_043_328
            ),
            cost_estimate=pl.CostEstimate(flops=flops, bytes_accessed=10 * tokens * d, transcendentals=tokens * ff),
            name="mlp_backward",
        )(x, dy, pre, w_in, w_down)
        last = last[: len(RINGS)]
        hops = [[(device(c, i, k), device(c, i + way, k)) for i in range(n)] for c, way in RINGS]
        came = [lax.ppermute(t, "tp", hop) for t, hop in zip(last, hops)]
        dw_in, dw_down = settle(dw_in, dw_down)
        return finish(own_term, *came), dw_in, dw_down

    rows = P(("dp", "tp"), None)
    return jax.shard_map(
        local,
        mesh=mesh,
        in_specs=(rows, rows, P("dp", "tp"), P(None, "tp"), P("tp", None)),
        out_specs=(rows, P("dp", "tp"), rows),
        check_vma=False,
    )
```
